32 devices in a mesh: dp: 4 (over z), space: 8 (over y, x, core).
Axes of the slice: x: 2, y: 2, z: 4, core: 2. Of those that a mesh axis runs over, the one named last changes fastest.
Arguments:
- lateral3: bfloat16 [16, 32, 128, 256], P('dp', 'space'), may hold values from -1200 to 1200
- lateral4: bfloat16 [16, 16, 64, 256], P('dp', 'space'), may hold values from -1200 to 1200
- lateral5: bfloat16 [16, 8, 32, 256], P('dp', 'space'), may hold values from -1200 to 1200
- conv_weight3: bfloat16 [3, 3, 256, 256], P(None, None, None, ('dp', 'space')), may hold values from -0.125 to 0.125
- conv_weight4: bfloat16 [3, 3, 256, 256], P(None, None, None, ('dp', 'space')), may hold values from -0.125 to 0.125
- conv_weight5: bfloat16 [3, 3, 256, 256], P(None, None, None, ('dp', 'space')), may hold values from -0.125 to 0.125
- norm_gain3: float32 [256], replicated, may hold values from 0.1 to 1.9
- norm_shift3: float32 [256], replicated, may hold values from -3 to 3
- norm_gain4: float32 [256], replicated, may hold values from 0.1 to 1.9
- norm_shift4: float32 [256], replicated, may hold values from -3 to 3
- norm_gain5: float32 [256], replicated, may hold values from 0.1 to 1.9
- norm_shift5: float32 [256], replicated, may hold values from -3 to 3
Outputs:
- pyramid3: float32 [16, 32, 128, 256], P('dp', 'space')
- pyramid4: float32 [16, 16, 64, 256], P('dp', 'space')
- pyramid5: float32 [16, 8, 32, 256], P('dp', 'space')
The draws below stay inside these ranges and needn't reach their ends.
All inputs are finite; a program needn't handle non-finite values.
Results may differ from the reference program's by a relative error of at most 0.007.
Values may be sent and summed in bfloat16 or wider, within the bound.
No kernel may reach another device: no remote copies, remote signals or barrier semaphores. Data moves between devices by JAX's collectives and lax.ppermute only.
A program may use at most 64 MiB of HBM per device.

```python
import jax
import jax.numpy as jnp
from jax import lax

C = 256
G = 32
W3 = 128
H5 = 8
H4 = 16
H3 = 32
W4 = 64
W5 = 32
BATCH = 16


def lateral_field(key, image_count, row_count, column_count, channel_count):
    pattern_key, column_key = jax.random.split(key, 2)
    heights = jnp.arange(row_count, dtype=jnp.float32) / max(row_count - 1, 1)
    shape_full = (image_count, row_count, column_count, channel_count)
    pattern = jnp.clip(jax.random.normal(pattern_key, shape_full, jnp.float32), -6.0, 6.0)
    row_scale = 10.0 ** heights
    column_scale = 10.0 ** jax.random.uniform(column_key, (image_count, 1, column_count, 1), jnp.float32, 0.0, 1.0)
    return pattern * row_scale[None, :, None, None] * column_scale


def draw_lateral3(key, part):
    return lateral_field(jax.random.fold_in(key, 3), BATCH, H3, W3, C).astype(jnp.bfloat16)


def draw_lateral4(key, part):
    return lateral_field(jax.random.fold_in(key, 4), BATCH, H4, W4, C).astype(jnp.bfloat16)


def draw_lateral5(key, part):
    return lateral_field(jax.random.fold_in(key, 5), BATCH, H5, W5, C).astype(jnp.bfloat16)


def steps_of(rng, dims, shards, least, largest):
    loudness, own = 1.0, jax.random.fold_in(rng, 6)
    for dim, parts in shards:
        steps = jnp.exp(jax.random.uniform(jax.random.fold_in(own, dim), (parts,), jnp.float32, least / len(shards), largest / len(shards)))
        loudness = loudness * jnp.repeat(steps, dims[dim] // parts).reshape([-1 if axis == dim else 1 for axis in range(len(dims))])
    return loudness


def scatter_about(rng, extent, scale, reach, pieces=(), kind=jnp.bfloat16):
    entries = jax.random.normal(rng, extent, jnp.float32) * scale
    if len(pieces) > 0:
        entries = steps_of(rng, extent, pieces, -0.22, 0.18) * entries
    return jnp.clip(entries, min=-reach, max=reach).astype(kind)


def setup_inputs(seed: int = 0) -> dict:
    streams_of = jax.random.split(jax.random.key(seed), 13)
    lateral3 = draw_lateral3(jax.random.fold_in(streams_of[12], 71), 0)
    lateral4 = draw_lateral4(jax.random.fold_in(streams_of[12], 71), 0)
    lateral5 = draw_lateral5(jax.random.fold_in(streams_of[12], 71), 0)
    conv_weight3 = scatter_about(streams_of[3], (3, 3, C, C), (9 * C) ** -0.5, 0.125, ((3, 32),))
    conv_weight4 = scatter_about(streams_of[4], (3, 3, C, C), (9 * C) ** -0.5, 0.125, ((3, 32),))
    conv_weight5 = scatter_about(streams_of[5], (3, 3, C, C), (9 * C) ** -0.5, 0.125, ((3, 32),))
    norm_gain3 = jnp.clip(1.0 + 0.18 * jax.random.normal(streams_of[6], (C,), jnp.float32), 0.1, 1.9)
    norm_shift3 = scatter_about(streams_of[7], (C,), 0.5, 3.0, (), jnp.float32)
    norm_gain4 = jnp.clip(1.0 + 0.18 * jax.random.normal(streams_of[8], (C,), jnp.float32), 0.1, 1.9)
    norm_shift4 = scatter_about(streams_of[9], (C,), 0.5, 3.0, (), jnp.float32)
    norm_gain5 = jnp.clip(1.0 + 0.18 * jax.random.normal(streams_of[10], (C,), jnp.float32), 0.1, 1.9)
    norm_shift5 = scatter_about(streams_of[11], (C,), 0.5, 3.0, (), jnp.float32)
    return {"lateral3": lateral3, "lateral4": lateral4, "lateral5": lateral5, "conv_weight3": conv_weight3, "conv_weight4": conv_weight4, "conv_weight5": conv_weight5, "norm_gain3": norm_gain3, "norm_shift3": norm_shift3, "norm_gain4": norm_gain4, "norm_shift4": norm_shift4, "norm_gain5": norm_gain5, "norm_shift5": norm_shift5}


epsilon = 1e-05

def enlarge(values):
    return jnp.repeat(jnp.repeat(values, 2, axis=0), 2, axis=1)

def convolve(single, kernel):
    result = lax.conv_general_dilated(single[None], kernel, (1, 1), ((1, 1), (1, 1)), dimension_numbers=('NHWC', 'HWIO', 'NHWC'), preferred_element_type=jnp.float32)
    return result[0]

def group_norm(values, gain_vector, shift_vector):
    blocks = values.reshape(values.shape[0], values.shape[1], G, values.shape[2] // G)
    center = lax.optimization_barrier(jnp.mean(blocks, axis=(0, 1, 3), keepdims=True))
    deviation = blocks - center
    spread = lax.optimization_barrier(jnp.mean(deviation * deviation, axis=(0, 1, 3), keepdims=True))
    scaled = deviation * lax.rsqrt(spread + epsilon)
    return scaled.reshape(values.shape) * gain_vector + shift_vector

def reference(lateral3, lateral4, lateral5, conv_weight3, conv_weight4, conv_weight5, norm_gain3, norm_shift3, norm_gain4, norm_shift4, norm_gain5, norm_shift5):

    def single_image(triple):
        fine_in, middle_in, coarse_in = triple
        merged5 = coarse_in
        merged4 = (middle_in.astype(jnp.float32) + enlarge(merged5).astype(jnp.float32)).astype(jnp.bfloat16)
        merged3 = (fine_in.astype(jnp.float32) + enlarge(merged4).astype(jnp.float32)).astype(jnp.bfloat16)
        output3 = group_norm(convolve(merged3, conv_weight3), norm_gain3, norm_shift3)
        output4 = group_norm(convolve(merged4, conv_weight4), norm_gain4, norm_shift4)
        output5 = group_norm(convolve(merged5, conv_weight5), norm_gain5, norm_shift5)
        return (output3, output4, output5)
    pyramid3, pyramid4, pyramid5 = lax.map(single_image, (lateral3, lateral4, lateral5))
    return (pyramid3, pyramid4, pyramid5)
```

```python
import functools

import jax
import jax.numpy as jnp
from jax import lax
from jax.experimental import pallas as pl
from jax.experimental.pallas import tpu as pltpu
from jax.sharding import PartitionSpec as P

G = 32
EPSILON = 1e-05
LANES = 128
AXES = ("dp", "space")
F32 = jnp.float32
BF16 = jnp.bfloat16
VMEM = pl.BlockSpec(memory_space=pltpu.VMEM)
ANY = pl.BlockSpec(memory_space=pl.ANY)


def exchange(array, axes, size, mask):
    return lax.ppermute(array, axes, [(i, i ^ mask) for i in range(size)])


def joined(first, second):
    return jnp.concatenate([first, second], axis=0)


def gathered_by_doubling(shards, bits):
    size = lax.axis_size(AXES)
    lead, turning = bits[:-3], bits[-3:]
    swap = functools.partial(exchange, axes=AXES, size=size)
    lengths = [s.shape[0] for s in shards]
    together = jnp.concatenate(shards, axis=0)[None]
    masks = [0]
    for bit in lead:
        together = joined(together, swap(together, mask=bit))
        masks = masks + [m ^ bit for m in masks]
    chunks, start = [], 0
    for length in lengths:
        chunks.append(together[:, start : start + length])
        start += length
    orders = [[turning[(k + step) % 3] for step in range(3)] for k in range(len(chunks))]
    held = [list(masks) for _ in chunks]
    for step in range(2):
        received = [swap(c, mask=o[step]) for c, o in zip(chunks, orders)]
        chunks = [joined(c, r) for c, r in zip(chunks, received)]
        held = [h + [m ^ o[step] for m in h] for h, o in zip(held, orders)]
    result = []
    for chunk, order, owner in zip(chunks, orders, held):
        received = swap(chunk, mask=order[2])
        parts = [chunk, received, swap(chunk, mask=1), swap(received, mask=1)]
        owners = [owner] + [[m ^ x for m in owner] for x in (order[2], 1, order[2] ^ 1)]
        result.append((parts, owners))
    return result


def weight_parts(weights):
    size = lax.axis_size(AXES)
    shards = []
    for weight in weights:
        rows, columns, inner, outer = weight.shape
        shards.append(jnp.transpose(weight, (0, 1, 3, 2)).reshape(rows * columns, outer, inner))
    bits = [1 << k for k in range(size.bit_length() - 1)][::-1][:-1]
    if size == 2 << (len(bits)) and len(bits) >= 3 and shards[0].shape[1] % 8 == 0:
        return gathered_by_doubling(shards, bits)
    result = []
    for shard in shards:
        whole = lax.all_gather(shard, AXES, axis=1, tiled=True)
        taps, outer, inner = whole.shape
        blocks = jnp.transpose(whole.reshape(taps, outer // 8, 8, inner), (1, 0, 2, 3))
        result.append(([blocks], None))
    return result


def halos(top, bottom):
    count = lax.axis_size("space")
    before = lax.ppermute(bottom, "space", [(i, i + 1) for i in range(count - 1)])
    after = lax.ppermute(top, "space", [(i + 1, i) for i in range(count - 1)])
    return before, after


def statistics_of_all(own):
    size = lax.axis_size("space")
    swap = functools.partial(exchange, axes="space", size=size)
    bits = [1 << k for k in range(size.bit_length() - 1)]
    if size != 1 << len(bits):
        return [lax.all_gather(own, "space")]
    held = [own[None]]
    for start in range(0, len(bits), 2) if len(bits) % 2 == 0 else [-1] + list(range(1, len(bits), 2)):
        some = bits[max(start, 0) : start + 2]
        whole = held[0] if len(held) == 1 else jnp.concatenate(held, axis=0)
        masks = some if len(some) == 1 else some + [some[0] | some[1]]
        held = [whole] + [swap(whole, mask=m) for m in masks]
    return held


def call(body, outs, ins, scratch, flops, in_specs=None, out_specs=None):
    moved = sum(a.size * a.dtype.itemsize for a in list(outs) + list(ins))
    return pl.pallas_call(
        body,
        out_shape=outs,
        in_specs=in_specs or [VMEM] * len(ins),
        out_specs=out_specs or [VMEM] * len(outs),
        scratch_shapes=scratch,
        cost_estimate=pl.CostEstimate(flops=flops, bytes_accessed=moved, transcendentals=0),
    )(*ins)


def stretched(scratch, values):
    rows = values.shape[0]
    pieces = []
    for k in range(scratch.shape[0]):
        piece = values[:, k * LANES : (k + 1) * LANES]
        scratch[k, pl.ds(0, rows, stride=2), :] = piece
        scratch[k, pl.ds(1, rows, stride=2), :] = piece
        pieces.append(scratch[k])
    return jnp.concatenate(pieces, axis=1)


def merge_body(l3, l4, l5, m3, m4, top, bottom, fine, middle):
    images, rows5 = l5.shape[0], l5.shape[1]
    for b in range(images):
        for r5 in range(rows5):
            up5 = stretched(middle, l5[b, r5].astype(F32))
            for r4 in (2 * r5, 2 * r5 + 1):
                v4 = (l4[b, r4].astype(F32) + up5).astype(BF16)
                m4[b, r4] = v4
                up4 = stretched(fine, v4.astype(F32))
                for r3 in (2 * r4, 2 * r4 + 1):
                    m3[b, r3] = (l3[b, r3].astype(F32) + up4).astype(BF16)
        start = 0
        for source in (m3, m4, l5):
            width = source.shape[2]
            top[b, start : start + width] = source[b, 0]
            bottom[b, start : start + width] = source[b, source.shape[1] - 1]
            start += width


def merge(l3, l4, l5):
    images, _, width3, channels = l3.shape
    width = width3 + l4.shape[2] + l5.shape[2]
    edge = jax.ShapeDtypeStruct((images, width, channels), BF16)
    outs = [jax.ShapeDtypeStruct(l3.shape, BF16), jax.ShapeDtypeStruct(l4.shape, BF16), edge, edge]
    scratch = [pltpu.VMEM((channels // LANES, w, LANES), F32) for w in (width3, l4.shape[2])]
    return call(merge_body, outs, [l3, l4, l5], scratch, 4 * l3.size)


def spread_body(m3, m4, l5, before, after, x3, x4, x5):
    start = 0
    for source, target in ((m3, x3), (m4, x4), (l5, x5)):
        images, rows, width, channels = source.shape
        place = lax.broadcasted_iota(jnp.int32, (width, channels), 0)
        for r in range(rows + 2):
            for b in range(images):
                if r == 0:
                    middle = before[b, start : start + width]
                elif r == rows + 1:
                    middle = after[b, start : start + width]
                else:
                    middle = source[b, r - 1]
                wide = middle.astype(F32)
                left = jnp.where(place == 0, 0.0, pltpu.roll(wide, 1, 0))
                right = jnp.where(place == width - 1, 0.0, pltpu.roll(wide, width - 1, 0))
                target[b, r, :, 0:channels] = left.astype(BF16)
                target[b, r, :, channels : 2 * channels] = middle
                target[b, r, :, 2 * channels : 3 * channels] = right.astype(BF16)
        start += width


def spread(levels, before, after):
    outs = [
        jax.ShapeDtypeStruct((a.shape[0], a.shape[1] + 2, a.shape[2], 3 * a.shape[3]), BF16)
        for a in levels
    ]
    return call(spread_body, outs, list(levels) + [before, after], [], 8 * sum(o.size for o in outs))


def conv_body(counts, owners, me_ref, *refs):
    levels = len(counts)
    refs = list(refs)
    xs, refs = refs[:levels], refs[levels:]
    parts = []
    for count in counts:
        parts.append(refs[:count])
        refs = refs[count:]
    outs, stats, blocks, kernel = refs[:levels], refs[levels], refs[levels + 1], refs[levels + 2]
    me = me_ref[0]
    taps, block_count, block, inner = blocks.shape
    for level in range(levels):
        x, out = xs[level], outs[level]
        base = 0
        for k, part in enumerate(parts[level]):
            for j in range(part.shape[0]):
                if owners[level] is None:
                    blocks[:, base + j] = part[j]
                else:
                    per = part.shape[2] // block
                    owner = me ^ owners[level][k][j]
                    for i in range(per):
                        blocks[:, owner * per + i] = part[j, :, i * block : (i + 1) * block]
            base += part.shape[0]
        for tap in range(taps):
            kernel[:, tap * inner : (tap + 1) * inner] = blocks[tap].reshape(block_count * block, inner)
        images, rows, width, outer = out.shape
        area = rows * width
        group = max(1, min(images, 512 // area))
        while images % group:
            group -= 1
        for b in range(0, images, group):
            wide = jnp.concatenate(
                [x[b : b + group, a : a + rows].reshape(group * area, 3 * inner) for a in range(3)],
                axis=1,
            )
            value = lax.dot_general(
                wide, kernel[...], (((1,), (1,)), ((), ())), preferred_element_type=F32
            )
            out[b : b + group] = value.reshape(group, rows, width, outer)
            for i in range(group):
                mine = value[i * area : (i + 1) * area]
                mean = jnp.sum(mine, axis=0, keepdims=True) * (1.0 / area)
                deviation = mine - mean
                line = level * 2 * images + b + i
                stats[line : line + 1] = mean
                stats[line + images : line + images + 1] = jnp.sum(
                    deviation * deviation, axis=0, keepdims=True
                )


def convolve(me, xs, weights):
    inner = xs[0].shape[3] // 3
    sample = weights[0][0][0]
    outer = sum(p.shape[0] * p.shape[2] for p in weights[0][0])
    outs = [
        jax.ShapeDtypeStruct((x.shape[0], x.shape[1] - 2, x.shape[2], outer), F32) for x in xs
    ]
    flops = sum(2 * o.size * 9 * inner for o in outs)
    outs.append(jax.ShapeDtypeStruct((2 * xs[0].shape[0] * len(xs), outer), F32))
    body = functools.partial(
        conv_body, [len(w[0]) for w in weights], [w[1] for w in weights]
    )
    ins = [me] + list(xs) + [p for w in weights for p in w[0]]
    scratch = [
        pltpu.VMEM((sample.shape[1], outer // 8, 8, inner), BF16),
        pltpu.VMEM((outer, sample.shape[1] * inner), BF16),
    ]
    specs = [pl.BlockSpec(memory_space=pltpu.SMEM)] + [VMEM] * (len(ins) - 1)
    result = call(body, outs, ins, scratch, flops, in_specs=specs)
    return result[:-1], result[-1]


def group_sums(values, size):
    lanes = values.shape[1]
    lane = lax.broadcasted_iota(jnp.int32, values.shape, 1)
    step = 1
    while step < size:
        up, down = pltpu.roll(values, lanes - step, 1), pltpu.roll(values, step, 1)
        values = values + jnp.where((lane & step) == 0, up, down)
        step *= 2
    return values


def norm_body(levels, pieces, *refs):
    refs = list(refs)
    xs, refs = refs[:levels], refs[levels:]
    affine, refs = refs[: 2 * levels], refs[2 * levels :]
    stats, refs = refs[:pieces], refs[pieces:]
    outs, refs = refs[:levels], refs[levels:]
    ys, sems = refs[:levels], refs[levels]
    images = xs[0].shape[0]
    channels = xs[0].shape[3]
    size = channels // G
    strips = [s[i] for s in stats for i in range(s.shape[0])]
    count = len(strips) * size
    total = group_sums(functools.reduce(jnp.add, strips), size)
    centers = total * (1.0 / count)
    apart = [(s - centers) for s in strips]
    between = group_sums(functools.reduce(jnp.add, [a * a for a in apart]), size)
    copies = []
    for level in range(levels):
        x, y = xs[level], ys[level]
        area = x.shape[1] * x.shape[2]
        first = level * 2 * images
        center = centers[first : first + images]
        spread = (
            total[first + images : first + 2 * images] + between[first : first + images] * area
        ) * (1.0 / (count * area))
        scale = lax.rsqrt(spread + EPSILON) * affine[2 * level][...]
        shift = affine[2 * level + 1][...]
        for b in range(images):
            flat = x[b].reshape(area, channels)
            line = (flat - center[b : b + 1]) * scale[b : b + 1] + shift
            y[b] = line.reshape(x.shape[1:])
            copy = pltpu.make_async_copy(y.at[b], outs[level].at[b], sems.at[level * images + b])
            copy.start()
            copies.append(copy)
    for copy in copies:
        copy.wait()


def normalize(xs, affine, stats):
    outs = [jax.ShapeDtypeStruct(x.shape, F32) for x in xs]
    ins = list(xs) + list(affine) + list(stats)
    scratch = [pltpu.VMEM(x.shape, F32) for x in xs]
    scratch.append(pltpu.SemaphoreType.DMA((len(xs) * xs[0].shape[0],)))
    body = functools.partial(norm_body, len(xs), len(stats))
    return call(
        body, outs, ins, scratch, 8 * sum(x.size for x in xs), out_specs=[ANY] * len(outs)
    )


def local(l3, l4, l5, w3, w4, w5, gain3, shift3, gain4, shift4, gain5, shift5):
    weights = weight_parts([w3, w4, w5])
    m3, m4, top, bottom = merge(l3, l4, l5)
    before, after = halos(top, bottom)
    x3, x4, x5 = spread((m3, m4, l5), before, after)
    me = lax.axis_index(AXES).astype(jnp.int32).reshape(1)
    (f3,), stats3 = convolve(me, [x3], weights[:1])
    (f4,), stats4 = convolve(me, [x4], weights[1:2])
    (f5,), stats5 = convolve(me, [x5], weights[2:])
    stats = statistics_of_all(jnp.concatenate([stats3, stats4, stats5], axis=0))
    affine = [a[None] for a in (gain3, shift3, gain4, shift4, gain5, shift5)]
    return tuple(normalize([f3, f4, f5], affine, stats))


def solution(mesh):
    image = P("dp", "space", None, None)
    weight = P(None, None, None, AXES)
    return jax.shard_map(
        local,
        mesh=mesh,
        in_specs=(image,) * 3 + (weight,) * 3 + (P(),) * 6,
        out_specs=(image,) * 3,
        check_vma=False,
    )
```

```python
import functools

import jax
import jax.numpy as jnp
from jax import lax
from jax.experimental import pallas as pl
from jax.experimental.pallas import tpu as pltpu
from jax.sharding import PartitionSpec as P


G = 32
EPSILON = 1e-05
LANES = 128
AXES = ("dp", "space")
F32 = jnp.float32
BF16 = jnp.bfloat16
VMEM = pl.BlockSpec(memory_space=pltpu.VMEM)
ANY = pl.BlockSpec(memory_space=pl.ANY)


def exchange(array, axes, size, masks):
    return lax.ppermute(array, axes, [(i, i ^ masks[i % 2]) for i in range(size)])


def joined(first, second):
    return jnp.concatenate([first, second], axis=0)


def gathered_in_chains(shards, bits):
    size = lax.axis_size(AXES)
    lead, (p, q, r) = bits[:-3], bits[-3:]
    lengths = [s.shape[0] for s in shards]
    together = jnp.concatenate(shards, axis=0)[None]
    for k, bit in enumerate(lead):
        received = exchange(together, AXES, size, (bit, bit))
        if k + 1 < len(lead):
            together = joined(together, received)
    cut = lengths[0]
    halves = [(together[:, :cut], received[:, :cut]), (together[:, cut:], received[:, cut:])]
    orders = [[(q, r), (r, q), (p, p)], [(p, p), (q, r), (r, q)]]
    swapped = [(len(lead), len(lead) + 1), (len(lead) + 1, len(lead) + 2)]
    result = []
    for pair, order, places, members in zip(
        halves, orders, swapped, (range(1), range(1, len(shards)))
    ):
        chunk = joined(*pair)
        for step in (0, 1):
            received = exchange(chunk, AXES, size, order[step])
            chunk = joined(chunk, received)
        received = exchange(chunk, AXES, size, order[2])
        near = exchange(chunk, AXES, size, (1, 1))
        far = exchange(received, AXES, size, (1, 1))
        steps = [(bit, bit) for bit in lead] + order
        start = 0
        for k in members:
            result.append(([chunk, received, near, far], start, steps, places))
            start += lengths[k]
    return result


def weight_parts(weights):
    size = lax.axis_size(AXES)
    shards = []
    for weight in weights:
        rows, columns, inner, outer = weight.shape
        shards.append(jnp.transpose(weight, (0, 1, 3, 2)).reshape(rows * columns, outer, inner))
    bits = [1 << k for k in range(size.bit_length() - 1)][::-1][:-1]
    paired = lax.axis_size("space") % 2 == 0
    if paired and size == 2 << len(bits) and len(bits) > 3 and shards[0].shape[1] == 8:
        return gathered_in_chains(shards, bits)
    return [
        ([lax.all_gather(shard, AXES, axis=1, tiled=True)], 0, None, None) for shard in shards
    ]


def halos(top, bottom):
    count = lax.axis_size("space")
    before = lax.ppermute(bottom, "space", [(i, i + 1) for i in range(count - 1)])
    after = lax.ppermute(top, "space", [(i + 1, i) for i in range(count - 1)])
    return before, after


def statistics_of_all(own):
    size = lax.axis_size("space")
    bits = [1 << k for k in range(size.bit_length() - 1)]
    if size != 1 << len(bits):
        return [lax.all_gather(own, "space")]
    held = [own[None]]
    for start in range(0, len(bits), 2) if len(bits) % 2 == 0 else [-1] + list(range(1, len(bits), 2)):
        some = bits[max(start, 0) : start + 2]
        whole = held[0] if len(held) == 1 else jnp.concatenate(held, axis=0)
        masks = some if len(some) == 1 else some + [some[0] | some[1]]
        held = [whole] + [exchange(whole, "space", size, (m, m)) for m in masks]
    return held


def call(body, outs, ins, scratch, flops, in_specs=None, out_specs=None):
    moved = sum(a.size * a.dtype.itemsize for a in list(outs) + list(ins))
    return pl.pallas_call(
        body,
        out_shape=outs,
        in_specs=in_specs or [VMEM] * len(ins),
        out_specs=out_specs or [VMEM] * len(outs),
        scratch_shapes=scratch,
        compiler_params=pltpu.CompilerParams(vmem_limit_bytes=20 << 20),
        cost_estimate=pl.CostEstimate(flops=flops, bytes_accessed=moved, transcendentals=0),
    )(*ins)


def stretched(scratch, values):
    rows = values.shape[0]
    pieces = []
    for k in range(scratch.shape[0]):
        piece = values[:, k * LANES : (k + 1) * LANES]
        scratch[k, pl.ds(0, rows, stride=2), :] = piece
        scratch[k, pl.ds(1, rows, stride=2), :] = piece
        pieces.append(scratch[k])
    return jnp.concatenate(pieces, axis=1)


def merge_body(l3, l4, l5, m3, m4, top, bottom, fine, middle):
    images, rows5 = l5.shape[0], l5.shape[1]
    for b in range(images):
        for r5 in range(rows5):
            up5 = stretched(middle, l5[b, r5].astype(F32))
            for r4 in (2 * r5, 2 * r5 + 1):
                v4 = (l4[b, r4].astype(F32) + up5).astype(BF16)
                m4[b, r4] = v4
                up4 = stretched(fine, v4.astype(F32))
                for r3 in (2 * r4, 2 * r4 + 1):
                    m3[b, r3] = (l3[b, r3].astype(F32) + up4).astype(BF16)
        start = 0
        for source in (m3, m4, l5):
            width = source.shape[2]
            top[b, start : start + width] = source[b, 0]
            bottom[b, start : start + width] = source[b, source.shape[1] - 1]
            start += width


def merge(l3, l4, l5):
    images, _, width3, channels = l3.shape
    width = width3 + l4.shape[2] + l5.shape[2]
    edge = jax.ShapeDtypeStruct((images, width, channels), BF16)
    outs = [jax.ShapeDtypeStruct(l3.shape, BF16), jax.ShapeDtypeStruct(l4.shape, BF16), edge, edge]
    scratch = [pltpu.VMEM((channels // LANES, w, LANES), F32) for w in (width3, l4.shape[2])]
    return call(merge_body, outs, [l3, l4, l5], scratch, 4 * l3.size)


def spread_body(m3, m4, l5, before, after, x3, x4, x5):
    start = 0
    for source, target in ((m3, x3), (m4, x4), (l5, x5)):
        images, rows, width, channels = source.shape
        place = lax.broadcasted_iota(jnp.int32, (width, channels), 0)
        for r in range(rows + 2):
            for b in range(images):
                if r == 0:
                    middle = before[b, start : start + width]
                elif r == rows + 1:
                    middle = after[b, start : start + width]
                else:
                    middle = source[b, r - 1]
                wide = middle.astype(F32)
                left = jnp.where(place == 0, 0.0, pltpu.roll(wide, 1, 0))
                right = jnp.where(place == width - 1, 0.0, pltpu.roll(wide, width - 1, 0))
                target[b, r, :, 0:channels] = left.astype(BF16)
                target[b, r, :, channels : 2 * channels] = middle
                target[b, r, :, 2 * channels : 3 * channels] = right.astype(BF16)
        start += width


def spread(levels, before, after):
    outs = [
        jax.ShapeDtypeStruct((a.shape[0], a.shape[1] + 2, a.shape[2], 3 * a.shape[3]), BF16)
        for a in levels
    ]
    return call(spread_body, outs, list(levels) + [before, after], [], 8 * sum(o.size for o in outs))


def lay_out(kernel, parts, start, steps, places, me, taps):
    inner = kernel.shape[1] // taps
    if steps is None:
        for tap in range(taps):
            kernel[:, tap * inner : (tap + 1) * inner] = parts[0][tap]
        return
    held, received, near, far = parts
    block = held.shape[2]
    core = me & 1
    depth = len(steps)
    first, second = places
    for j in range(1 << depth):
        flags = [(j >> k) & 1 for k in range(depth)]
        even = sum(step[0] for step, flag in zip(steps, flags) if flag)
        odd = sum(step[1] for step, flag in zip(steps, flags) if flag)
        chip = (me ^ (even + core * (odd - even))) >> 1
        other = list(flags)
        other[first], other[second] = flags[second], flags[first]
        place = sum(flag << k for k, flag in enumerate(other[:-1]))
        mine = (received if flags[-1] else held)[j % (1 << (depth - 1)), start : start + taps]
        theirs = (far if other[-1] else near)[place, start : start + taps]
        mine, theirs = mine.astype(F32), theirs.astype(F32)
        low, high = jnp.where(core == 0, mine, theirs), jnp.where(core == 0, theirs, mine)
        both = jnp.concatenate([low, high], axis=1).astype(BF16)
        row = pl.multiple_of(chip * (2 * block), 2 * block)
        for tap in range(taps):
            kernel[pl.ds(row, 2 * block), tap * inner : (tap + 1) * inner] = both[tap]


def conv_body(counts, layouts, me_ref, *refs):
    levels = len(layouts)
    refs = list(refs)
    xs, refs = refs[:levels], refs[levels:]
    parts, refs = refs[:counts], refs[counts:]
    outs, stats, kernels = refs[:levels], refs[levels], refs[levels + 1 :]
    me = me_ref[0]
    for level in range(levels):
        x, out, kernel = xs[level], outs[level], kernels[level]
        first, last, start, steps, places = layouts[level]
        inner = x.shape[3] // 3
        lay_out(kernel, parts[first:last], start, steps, places, me, kernel.shape[1] // inner)
        images, rows, width, outer = out.shape
        area = rows * width
        group = max(1, min(images, 512 // area))
        while images % group:
            group -= 1
        for b in range(0, images, group):
            wide = jnp.concatenate(
                [x[b : b + group, a : a + rows].reshape(group * area, 3 * inner) for a in range(3)],
                axis=1,
            )
            value = lax.dot_general(
                wide, kernel[...], (((1,), (1,)), ((), ())), preferred_element_type=F32
            )
            out[b : b + group] = value.reshape(group, rows, width, outer)
            for i in range(group):
                mine = value[i * area : (i + 1) * area]
                mean = jnp.sum(mine, axis=0, keepdims=True) * (1.0 / area)
                deviation = mine - mean
                line = level * 2 * images + b + i
                stats[line : line + 1] = mean
                stats[line + images : line + images + 1] = jnp.sum(
                    deviation * deviation, axis=0, keepdims=True
                )


def convolve(me, xs, weights, outer):
    inner = xs[0].shape[3] // 3
    outs = [
        jax.ShapeDtypeStruct((x.shape[0], x.shape[1] - 2, x.shape[2], outer), F32) for x in xs
    ]
    flops = sum(2 * o.size * 9 * inner for o in outs)
    outs.append(jax.ShapeDtypeStruct((2 * xs[0].shape[0] * len(xs), outer), F32))
    arrays, layouts, before = [], [], None
    for parts, start, steps, places in weights:
        if parts is not before:
            arrays.extend(parts)
        before = parts
        layouts.append((len(arrays) - len(parts), len(arrays), start, steps, places))
    body = functools.partial(conv_body, len(arrays), layouts)
    ins = [me] + list(xs) + arrays
    scratch = [pltpu.VMEM((outer, 9 * inner), BF16) for _ in xs]
    specs = [pl.BlockSpec(memory_space=pltpu.SMEM)] + [VMEM] * (len(ins) - 1)
    result = call(body, outs, ins, scratch, flops, in_specs=specs)
    return result[:-1], result[-1]


def group_sums(values, size):
    lanes = values.shape[1]
    lane = lax.broadcasted_iota(jnp.int32, values.shape, 1)
    step = 1
    while step < size:
        up, down = pltpu.roll(values, lanes - step, 1), pltpu.roll(values, step, 1)
        values = values + jnp.where((lane & step) == 0, up, down)
        step *= 2
    return values


def norm_body(levels, pieces, *refs):
    refs = list(refs)
    xs, refs = refs[:levels], refs[levels:]
    affine, refs = refs[: 2 * levels], refs[2 * levels :]
    stats, refs = refs[:pieces], refs[pieces:]
    outs, refs = refs[:levels], refs[levels:]
    ys, sems = refs[:levels], refs[levels]
    images = xs[0].shape[0]
    channels = xs[0].shape[3]
    size = channels // G
    strips = [s[i] for s in stats for i in range(s.shape[0])]
    count = len(strips) * size
    total = group_sums(functools.reduce(jnp.add, strips), size)
    centers = total * (1.0 / count)
    apart = [(s - centers) for s in strips]
    between = group_sums(functools.reduce(jnp.add, [a * a for a in apart]), size)
    copies = []
    for level in range(levels):
        x, y = xs[level], ys[level]
        area = x.shape[1] * x.shape[2]
        first = level * 2 * images
        center = centers[first : first + images]
        spread = (
            total[first + images : first + 2 * images] + between[first : first + images] * area
        ) * (1.0 / (count * area))
        scale = lax.rsqrt(spread + EPSILON) * affine[2 * level][...]
        shift = affine[2 * level + 1][...]
        for b in range(images):
            flat = x[b].reshape(area, channels)
            line = (flat - center[b : b + 1]) * scale[b : b + 1] + shift
            y[b] = line.reshape(x.shape[1:])
            copy = pltpu.make_async_copy(y.at[b], outs[level].at[b], sems.at[level * images + b])
            copy.start()
            copies.append(copy)
    for copy in copies:
        copy.wait()


def normalize(xs, affine, stats):
    outs = [jax.ShapeDtypeStruct(x.shape, F32) for x in xs]
    ins = list(xs) + list(affine) + list(stats)
    scratch = [pltpu.VMEM(x.shape, F32) for x in xs]
    scratch.append(pltpu.SemaphoreType.DMA((len(xs) * xs[0].shape[0],)))
    body = functools.partial(norm_body, len(xs), len(stats))
    return call(
        body, outs, ins, scratch, 8 * sum(x.size for x in xs), out_specs=[ANY] * len(outs)
    )


def local(l3, l4, l5, w3, w4, w5, gain3, shift3, gain4, shift4, gain5, shift5):
    weights = weight_parts([w3, w4, w5])
    outer = shift3.shape[0]
    m3, m4, top, bottom = merge(l3, l4, l5)
    before, after = halos(top, bottom)
    x3, x4, x5 = spread((m3, m4, l5), before, after)
    me = lax.axis_index(AXES).astype(jnp.int32).reshape(1)
    (f3,), stats3 = convolve(me, [x3], weights[:1], outer)
    (f4, f5), stats45 = convolve(me, [x4, x5], weights[1:], outer)
    stats = statistics_of_all(jnp.concatenate([stats3, stats45], axis=0))
    affine = [a[None] for a in (gain3, shift3, gain4, shift4, gain5, shift5)]
    return tuple(normalize([f3, f4, f5], affine, stats))


def solution(mesh):
    image = P("dp", "space", None, None)
    weight = P(None, None, None, AXES)
    return jax.shard_map(
        local,
        mesh=mesh,
        in_specs=(image,) * 3 + (weight,) * 3 + (P(),) * 6,
        out_specs=(image,) * 3,
        check_vma=False,
    )
```

```python
import functools

import jax
import jax.numpy as jnp
from jax import lax
from jax.experimental import pallas as pl
from jax.experimental.pallas import tpu as pltpu
from jax.sharding import PartitionSpec as P


G = 32
EPSILON = 1e-05
LANES = 128
AXES = ("dp", "space")
F32 = jnp.float32
BF16 = jnp.bfloat16
VMEM = pl.BlockSpec(memory_space=pltpu.VMEM)
ANY = pl.BlockSpec(memory_space=pl.ANY)


def exchange(array, axes, size, masks):
    return lax.ppermute(array, axes, [(i, i ^ masks[i % 2]) for i in range(size)])


def join_body(*refs):
    target, start = refs[-1], 0
    for ref in refs[:-1]:
        target[start : start + ref.shape[0]] = ref[...]
        start += ref.shape[0]


def joined(*arrays):
    count = sum(a.shape[0] for a in arrays)
    out = jax.ShapeDtypeStruct((count,) + arrays[0].shape[1:], arrays[0].dtype)
    return call(join_body, [out], list(arrays), [], out.size, room=1)[0]


def halve_body(cut, first, second, *targets):
    for target, lo, hi in ((targets[0], 0, cut), (targets[1], cut, first.shape[1])):
        count = first.shape[0]
        target[:count] = first[:, lo:hi]
        target[count:] = second[:, lo:hi]


def halved(first, second, cut):
    count, length = first.shape[:2]
    outs = [
        jax.ShapeDtypeStruct((2 * count, n) + first.shape[2:], first.dtype)
        for n in (cut, length - cut)
    ]
    return call(functools.partial(halve_body, cut), outs, [first, second], [], 2 * first.size, room=1)


def gathered_in_chains(together, lengths, bits):
    size = lax.axis_size(AXES)
    lead, (p, q, r) = bits[:-3], bits[-3:]
    for k, bit in enumerate(lead):
        received = exchange(together, AXES, size, (bit, bit))
        if k + 1 < len(lead):
            together = joined(together, received)
    chunks = halved(together, received, lengths[0])
    orders = [[(q, r), (r, q), (p, p)], [(p, p), (q, r), (r, q)]]
    swapped = [(len(lead), len(lead) + 1), (len(lead) + 1, len(lead) + 2)]
    result = []
    for chunk, order, places, members in zip(
        chunks, orders, swapped, (range(1), range(1, len(lengths)))
    ):
        for step in (0, 1):
            received = exchange(chunk, AXES, size, order[step])
            chunk = joined(chunk, received)
        received = exchange(chunk, AXES, size, order[2])
        near = exchange(chunk, AXES, size, (1, 1))
        far = exchange(received, AXES, size, (1, 1))
        steps = [(bit, bit) for bit in lead] + order
        start = 0
        for k in members:
            result.append(([chunk, received, near, far], start, steps, places))
            start += lengths[k]
    return result


def weight_parts(weights):
    size = lax.axis_size(AXES)
    shards = []
    for weight in weights:
        rows, columns, inner, outer = weight.shape
        shards.append(jnp.transpose(weight, (0, 1, 3, 2)).reshape(rows * columns, outer, inner))
    bits = [1 << k for k in range(size.bit_length() - 1)][::-1][:-1]
    paired = lax.axis_size("space") % 2 == 0
    if paired and size == 2 << len(bits) and len(bits) > 3 and shards[0].shape[1] == 8:
        together = jnp.concatenate(shards, axis=0)[None]
        return gathered_in_chains(together, [s.shape[0] for s in shards], bits)
    return [
        ([lax.all_gather(shard, AXES, axis=1, tiled=True)], 0, None, None) for shard in shards
    ]


def starts_of(*levels):
    starts, start = [], 0
    for level in levels:
        starts.append(start)
        start += level.shape[2]
    return starts


def halos(*levels):
    count = lax.axis_size("space")
    ahead = [(i, i + 1) for i in range(count - 1)]
    top = jnp.concatenate([a[:, 0] for a in levels], axis=1)
    bottom = jnp.concatenate([a[:, -1] for a in levels], axis=1)
    before = lax.ppermute(bottom, "space", ahead)
    after = lax.ppermute(top, "space", [(j, i) for i, j in ahead])
    return before, after


def statistics_of_all(own):
    size = lax.axis_size("space")
    bits = [1 << k for k in range(size.bit_length() - 1)]
    if size != 1 << len(bits):
        return [lax.all_gather(own, "space")]
    held = [own[None]]
    for start in range(0, len(bits), 2) if len(bits) % 2 == 0 else [-1] + list(range(1, len(bits), 2)):
        some = bits[max(start, 0) : start + 2]
        whole = held[0] if len(held) == 1 else joined(*held)
        masks = some if len(some) == 1 else some + [some[0] | some[1]]
        held = [whole] + [exchange(whole, "space", size, (m, m)) for m in masks]
    return held


def call(body, outs, ins, scratch, flops, in_specs=None, out_specs=None, room=8):
    moved = sum(a.size * a.dtype.itemsize for a in list(outs) + list(ins))
    return pl.pallas_call(
        body,
        out_shape=outs,
        in_specs=in_specs or [VMEM] * len(ins),
        out_specs=out_specs or [VMEM] * len(outs),
        scratch_shapes=scratch,
        compiler_params=pltpu.CompilerParams(vmem_limit_bytes=room << 20),
        cost_estimate=pl.CostEstimate(flops=flops, bytes_accessed=moved, transcendentals=0),
    )(*ins)


def stretched(scratch, values):
    rows = values.shape[0]
    pieces = []
    for k in range(scratch.shape[0]):
        piece = values[:, k * LANES : (k + 1) * LANES]
        scratch[k, pl.ds(0, rows, stride=2), :] = piece
        scratch[k, pl.ds(1, rows, stride=2), :] = piece
        pieces.append(scratch[k])
    return jnp.concatenate(pieces, axis=1)


def prepare_body(l3, l4, l5, before, after, x3, x4, x5, fine, middle):
    images, rows5 = l5.shape[0], l5.shape[1]
    channels = l5.shape[3]

    def put(target, b, row, wide):
        width = wide.shape[0]
        column = lax.broadcasted_iota(jnp.int32, wide.shape, 0)
        left = jnp.where(column == 0, 0.0, pltpu.roll(wide, 1, 0))
        right = jnp.where(column == width - 1, 0.0, pltpu.roll(wide, width - 1, 0))
        for k, piece in enumerate((left, wide, right)):
            target[b, row, :, k * channels : (k + 1) * channels] = piece.astype(BF16)

    def rounded(values):
        return values.astype(BF16).astype(F32)

    starts = starts_of(l3, l4, l5)
    for b in range(images):
        for side, halo in enumerate((before, after)):
            rows = []
            for source, start in zip((l3, l4, l5), starts):
                rows.append(halo[b, start : start + source.shape[2]].astype(F32))
            put(x5, b, side * (x5.shape[1] - 1), rows[2])
            v4 = rounded(rows[1] + stretched(middle, rows[2]))
            put(x4, b, side * (x4.shape[1] - 1), v4)
            put(x3, b, side * (x3.shape[1] - 1), rounded(rows[0] + stretched(fine, v4)))
        for r5 in range(rows5):
            v5 = l5[b, r5].astype(F32)
            put(x5, b, 1 + r5, v5)
            up5 = stretched(middle, v5)
            for r4 in (2 * r5, 2 * r5 + 1):
                v4 = rounded(l4[b, r4].astype(F32) + up5)
                put(x4, b, 1 + r4, v4)
                up4 = stretched(fine, v4)
                for r3 in (2 * r4, 2 * r4 + 1):
                    put(x3, b, 1 + r3, rounded(l3[b, r3].astype(F32) + up4))


def prepare(l3, l4, l5, before, after):
    levels = (l3, l4, l5)
    channels = l3.shape[3]
    outs = [
        jax.ShapeDtypeStruct((a.shape[0], a.shape[1] + 2, a.shape[2], 3 * channels), BF16)
        for a in levels
    ]
    scratch = [pltpu.VMEM((channels // LANES, a.shape[2], LANES), F32) for a in (l3, l4)]
    ins = [l3, l4, l5, before, after]
    return call(prepare_body, outs, ins, scratch, 8 * sum(o.size for o in outs), room=2)


def lay_out(kernel, parts, start, steps, places, me, taps):
    inner = kernel.shape[1] // taps
    if steps is None:
        for tap in range(taps):
            kernel[:, tap * inner : (tap + 1) * inner] = parts[0][tap]
        return
    held, received, near, far = parts
    block = held.shape[2]
    core = me & 1
    depth = len(steps)
    first, second = places
    for j in range(1 << depth):
        flags = [(j >> k) & 1 for k in range(depth)]
        even = sum(step[0] for step, flag in zip(steps, flags) if flag)
        odd = sum(step[1] for step, flag in zip(steps, flags) if flag)
        chip = (me ^ (even + core * (odd - even))) >> 1
        other = list(flags)
        other[first], other[second] = flags[second], flags[first]
        place = sum(flag << k for k, flag in enumerate(other[:-1]))
        mine = (received if flags[-1] else held)[j % (1 << (depth - 1)), start : start + taps]
        theirs = (far if other[-1] else near)[place, start : start + taps]
        mine, theirs = mine.astype(F32), theirs.astype(F32)
        low, high = jnp.where(core == 0, mine, theirs), jnp.where(core == 0, theirs, mine)
        both = jnp.concatenate([low, high], axis=1).astype(BF16)
        row = pl.multiple_of(chip * (2 * block), 2 * block)
        for tap in range(taps):
            kernel[pl.ds(row, 2 * block), tap * inner : (tap + 1) * inner] = both[tap]


def conv_body(counts, layouts, *refs):
    levels = len(layouts)
    refs = list(refs)
    xs, refs = refs[:levels], refs[levels:]
    parts, refs = refs[:counts], refs[counts:]
    outs, stats, kernels = refs[:levels], refs[levels], refs[levels + 1 :]
    me = lax.axis_index("dp") * lax.axis_size("space") + lax.axis_index("space")
    for level in range(levels):
        x, out, kernel = xs[level], outs[level], kernels[level]
        first, last, start, steps, places = layouts[level]
        inner = x.shape[3] // 3
        lay_out(kernel, parts[first:last], start, steps, places, me, kernel.shape[1] // inner)
        images, rows, width, outer = out.shape
        area = rows * width
        group = max(1, min(images, 512 // area))
        while images % group:
            group -= 1
        for b in range(0, images, group):
            wide = jnp.concatenate(
                [x[b : b + group, a : a + rows].reshape(group * area, 3 * inner) for a in range(3)],
                axis=1,
            )
            value = lax.dot_general(
                wide, kernel[...], (((1,), (1,)), ((), ())), preferred_element_type=F32
            )
            out[b : b + group] = value.reshape(group, rows, width, outer)
            for i in range(group):
                mine = value[i * area : (i + 1) * area]
                mean = jnp.sum(mine, axis=0, keepdims=True) * (1.0 / area)
                deviation = mine - mean
                line = level * 2 * images + b + i
                stats[line : line + 1] = mean
                stats[line + images : line + images + 1] = jnp.sum(
                    deviation * deviation, axis=0, keepdims=True
                )


def convolve(xs, weights, outer):
    inner = xs[0].shape[3] // 3
    outs = [
        jax.ShapeDtypeStruct((x.shape[0], x.shape[1] - 2, x.shape[2], outer), F32) for x in xs
    ]
    flops = sum(2 * o.size * 9 * inner for o in outs)
    outs.append(jax.ShapeDtypeStruct((2 * xs[0].shape[0] * len(xs), outer), F32))
    arrays, layouts, before = [], [], None
    for parts, start, steps, places in weights:
        if parts is not before:
            arrays.extend(parts)
        before = parts
        layouts.append((len(arrays) - len(parts), len(arrays), start, steps, places))
    body = functools.partial(conv_body, len(arrays), layouts)
    ins = list(xs) + arrays
    scratch = [pltpu.VMEM((outer, 9 * inner), BF16) for _ in xs]
    result = call(body, outs, ins, scratch, flops)
    return result[:-1], result[-1]


def group_sums(values, size):
    lanes = values.shape[1]
    lane = lax.broadcasted_iota(jnp.int32, values.shape, 1)
    step = 1
    while step < size:
        up, down = pltpu.roll(values, lanes - step, 1), pltpu.roll(values, step, 1)
        values = values + jnp.where((lane & step) == 0, up, down)
        step *= 2
    return values


def norm_body(levels, pieces, *refs):
    refs = list(refs)
    xs, refs = refs[:levels], refs[levels:]
    affine, refs = refs[: 2 * levels], refs[2 * levels :]
    stats, refs = refs[:pieces], refs[pieces:]
    outs, refs = refs[:levels], refs[levels:]
    ys, sems = refs[:levels], refs[levels]
    images = xs[0].shape[0]
    channels = xs[0].shape[3]
    size = channels // G
    strips = [s[i] for s in stats for i in range(s.shape[0])]
    count = len(strips) * size
    total = group_sums(functools.reduce(jnp.add, strips), size)
    centers = total * (1.0 / count)
    apart = [(s - centers) for s in strips]
    between = group_sums(functools.reduce(jnp.add, [a * a for a in apart]), size)
    copies = []
    for level in range(levels):
        x, y = xs[level], ys[level]
        area = x.shape[1] * x.shape[2]
        first = level * 2 * images
        center = centers[first : first + images]
        spread = (
            total[first + images : first + 2 * images] + between[first : first + images] * area
        ) * (1.0 / (count * area))
        scale = lax.rsqrt(spread + EPSILON) * affine[2 * level][...]
        shift = affine[2 * level + 1][...]
        for b in range(images):
            flat = x[b].reshape(area, channels)
            line = (flat - center[b : b + 1]) * scale[b : b + 1] + shift
            y[b] = line.reshape(x.shape[1:])
            copy = pltpu.make_async_copy(y.at[b], outs[level].at[b], sems.at[level * images + b])
            copy.start()
            copies.append(copy)
    for copy in copies:
        copy.wait()


def normalize(xs, affine, stats):
    outs = [jax.ShapeDtypeStruct(x.shape, F32) for x in xs]
    ins = list(xs) + list(affine) + list(stats)
    scratch = [pltpu.VMEM(x.shape, F32) for x in xs]
    scratch.append(pltpu.SemaphoreType.DMA((len(xs) * xs[0].shape[0],)))
    body = functools.partial(norm_body, len(xs), len(stats))
    return call(
        body, outs, ins, scratch, 8 * sum(x.size for x in xs), out_specs=[ANY] * len(outs)
    )


def local(l3, l4, l5, w3, w4, w5, gain3, shift3, gain4, shift4, gain5, shift5):
    weights = weight_parts([w3, w4, w5])
    outer = shift3.shape[0]
    before, after = halos(l3, l4, l5)
    x3, x4, x5 = prepare(l3, l4, l5, before, after)
    (f3,), stats3 = convolve([x3], weights[:1], outer)
    (f4, f5), stats45 = convolve([x4, x5], weights[1:], outer)
    stats = statistics_of_all(joined(stats3, stats45))
    affine = [a[None] for a in (gain3, shift3, gain4, shift4, gain5, shift5)]
    return tuple(normalize([f3, f4, f5], affine, stats))


def solution(mesh):
    image = P("dp", "space", None, None)
    weight = P(None, None, None, AXES)
    return jax.shard_map(
        local,
        mesh=mesh,
        in_specs=(image,) * 3 + (weight,) * 3 + (P(),) * 6,
        out_specs=(image,) * 3,
        check_vma=False,
    )
```

```python
import functools

import jax
import jax.numpy as jnp
from jax import lax
from jax.experimental import pallas as pl
from jax.experimental.pallas import tpu as pltpu
from jax.sharding import PartitionSpec as P


G = 32
EPSILON = 1e-05
LANES = 128
AXES = ("dp", "space")
F32 = jnp.float32
BF16 = jnp.bfloat16
VMEM = pl.BlockSpec(memory_space=pltpu.VMEM)
ANY = pl.BlockSpec(memory_space=pl.ANY)


def exchange(array, axes, size, masks):
    return lax.ppermute(array, axes, [(i, i ^ masks[i % 2]) for i in range(size)])


def join_body(*refs):
    target, start = refs[-1], 0
    for ref in refs[:-1]:
        target[start : start + ref.shape[0]] = ref[...]
        start += ref.shape[0]


def joined(*arrays):
    count = sum(a.shape[0] for a in arrays)
    out = jax.ShapeDtypeStruct((count,) + arrays[0].shape[1:], arrays[0].dtype)
    return call(join_body, [out], list(arrays), [], out.size, room=1)[0]


def halve_body(cut, first, second, *targets):
    for target, lo, hi in ((targets[0], 0, cut), (targets[1], cut, first.shape[1])):
        count = first.shape[0]
        target[:count] = first[:, lo:hi]
        target[count:] = second[:, lo:hi]


def halved(first, second, cut):
    count, length = first.shape[:2]
    outs = [
        jax.ShapeDtypeStruct((2 * count, n) + first.shape[2:], first.dtype)
        for n in (cut, length - cut)
    ]
    return call(functools.partial(halve_body, cut), outs, [first, second], [], 2 * first.size, room=1)


def gathered_in_chains(together, lengths, bits):
    size = lax.axis_size(AXES)
    lead, (p, q, r) = bits[:-3], bits[-3:]
    for k, bit in enumerate(lead):
        received = exchange(together, AXES, size, (bit, bit))
        if k + 1 < len(lead):
            together = joined(together, received)
    chunks = halved(together, received, lengths[0])
    orders = [[(q, r), (r, q), (p, p)], [(p, p), (q, r), (r, q)]]
    swapped = [(len(lead), len(lead) + 1), (len(lead) + 1, len(lead) + 2)]
    result = []
    for chunk, order, places, members in zip(chunks, orders, swapped, (range(1), range(1, len(lengths)))):
        for step in (0, 1):
            received = exchange(chunk, AXES, size, order[step])
            chunk = joined(chunk, received)
        received = exchange(chunk, AXES, size, order[2])
        near = exchange(chunk, AXES, size, (1, 1))
        far = exchange(received, AXES, size, (1, 1))
        steps = [(bit, bit) for bit in lead] + order
        start = 0
        for k in members:
            result.append(([chunk, received, near, far], start, steps, places))
            start += lengths[k]
    return result


def weight_parts(weights):
    size = lax.axis_size(AXES)
    shards = []
    for weight in weights:
        rows, columns, inner, outer = weight.shape
        shards.append(jnp.transpose(weight, (0, 1, 3, 2)).reshape(rows * columns, outer, inner))
    bits = [1 << k for k in range(size.bit_length() - 1)][::-1][:-1]
    paired = lax.axis_size("space") % 2 == 0
    if paired and size == 2 << len(bits) and len(bits) > 3 and shards[0].shape[1] == 8:
        together = jnp.concatenate(shards, axis=0)[None]
        return gathered_in_chains(together, [s.shape[0] for s in shards], bits)
    return [
        ([lax.all_gather(shard, AXES, axis=1, tiled=True)], 0, None, None) for shard in shards
    ]


def starts_of(*levels):
    starts, start = [], 0
    for level in levels:
        starts.append(start)
        start += level.shape[2]
    return starts


def edges_body(l3, l4, l5, top, bottom, sems):
    copies = []
    for source, start in zip((l3, l4, l5), starts_of(l3, l4, l5)):
        rows, width = source.shape[1:3]
        for target, row in ((top, 0), (bottom, rows - 1)):
            copies.append(
                pltpu.make_async_copy(
                    source.at[:, row], target.at[:, start : start + width], sems.at[len(copies)]
                )
            )
            copies[-1].start()
    for copy in copies:
        copy.wait()


def halos(*levels):
    count = lax.axis_size("space")
    ahead = [(i, i + 1) for i in range(count - 1)]
    width = sum(a.shape[2] for a in levels)
    edge = jax.ShapeDtypeStruct((levels[0].shape[0], width, levels[0].shape[3]), BF16)
    kept = [pltpu.with_memory_space_constraint(a, pltpu.HBM) for a in levels]
    scratch = [pltpu.SemaphoreType.DMA((2 * len(levels),))]
    top, bottom = call(
        edges_body, [edge, edge], kept, scratch, edge.size, in_specs=[ANY] * len(kept), room=1
    )
    before = lax.ppermute(bottom, "space", ahead)
    after = lax.ppermute(top, "space", [(j, i) for i, j in ahead])
    return before, after


def statistics_of_all(own):
    size = lax.axis_size("space")
    bits = [1 << k for k in range(size.bit_length() - 1)]
    if size != 1 << len(bits):
        return [lax.all_gather(own, "space")]
    held = [own[None]]
    for start in range(0, len(bits), 2) if len(bits) % 2 == 0 else [-1] + list(range(1, len(bits), 2)):
        some = bits[max(start, 0) : start + 2]
        whole = held[0] if len(held) == 1 else joined(*held)
        masks = some if len(some) == 1 else some + [some[0] | some[1]]
        held = [whole] + [exchange(whole, "space", size, (m, m)) for m in masks]
    return held


def call(body, outs, ins, scratch, flops, in_specs=None, out_specs=None, room=8):
    moved = sum(a.size * a.dtype.itemsize for a in list(outs) + list(ins))
    return pl.pallas_call(
        body,
        out_shape=outs,
        in_specs=in_specs or [VMEM] * len(ins),
        out_specs=out_specs or [VMEM] * len(outs),
        scratch_shapes=scratch,
        compiler_params=pltpu.CompilerParams(vmem_limit_bytes=room << 20),
        cost_estimate=pl.CostEstimate(flops=flops, bytes_accessed=moved, transcendentals=0),
    )(*ins)


def stretched(scratch, values):
    rows = values.shape[0]
    pieces = []
    for k in range(scratch.shape[0]):
        piece = values[:, k * LANES : (k + 1) * LANES]
        scratch[k, pl.ds(0, rows, stride=2), :] = piece
        scratch[k, pl.ds(1, rows, stride=2), :] = piece
        pieces.append(scratch[k])
    return jnp.concatenate(pieces, axis=1)


def prepare_body(l3, l4, l5, before, after, x3, x4, x5, fine, middle):
    images, rows5 = l5.shape[0], l5.shape[1]
    channels = l5.shape[3]

    def put(target, b, row, wide):
        width = wide.shape[0]
        column = lax.broadcasted_iota(jnp.int32, wide.shape, 0)
        left = jnp.where(column == 0, 0.0, pltpu.roll(wide, 1, 0))
        right = jnp.where(column == width - 1, 0.0, pltpu.roll(wide, width - 1, 0))
        for k, piece in enumerate((left, wide, right)):
            target[b, row, :, k * channels : (k + 1) * channels] = piece.astype(BF16)

    def rounded(values):
        return values.astype(BF16).astype(F32)

    starts = starts_of(l3, l4, l5)
    for b in range(images):
        for side, halo in enumerate((before, after)):
            rows = []
            for source, start in zip((l3, l4, l5), starts):
                rows.append(halo[b, start : start + source.shape[2]].astype(F32))
            put(x5, b, side * (x5.shape[1] - 1), rows[2])
            v4 = rounded(rows[1] + stretched(middle, rows[2]))
            put(x4, b, side * (x4.shape[1] - 1), v4)
            put(x3, b, side * (x3.shape[1] - 1), rounded(rows[0] + stretched(fine, v4)))
        for r5 in range(rows5):
            v5 = l5[b, r5].astype(F32)
            put(x5, b, 1 + r5, v5)
            up5 = stretched(middle, v5)
            for r4 in (2 * r5, 2 * r5 + 1):
                v4 = rounded(l4[b, r4].astype(F32) + up5)
                put(x4, b, 1 + r4, v4)
                up4 = stretched(fine, v4)
                for r3 in (2 * r4, 2 * r4 + 1):
                    put(x3, b, 1 + r3, rounded(l3[b, r3].astype(F32) + up4))


def prepare(l3, l4, l5, before, after):
    levels = (l3, l4, l5)
    channels = l3.shape[3]
    outs = [
        jax.ShapeDtypeStruct((a.shape[0], a.shape[1] + 2, a.shape[2], 3 * channels), BF16)
        for a in levels
    ]
    scratch = [pltpu.VMEM((channels // LANES, a.shape[2], LANES), F32) for a in (l3, l4)]
    ins = [l3, l4, l5, before, after]
    return call(prepare_body, outs, ins, scratch, 8 * sum(o.size for o in outs), room=2)


def lay_out(kernel, parts, start, steps, places, me, taps):
    inner = kernel.shape[1] // taps
    if steps is None:
        for tap in range(taps):
            kernel[:, tap * inner : (tap + 1) * inner] = parts[0][tap]
        return
    held, received, near, far = parts
    block = held.shape[2]
    core = me & 1
    depth = len(steps)
    first, second = places
    for j in range(1 << depth):
        flags = [(j >> k) & 1 for k in range(depth)]
        even = sum(step[0] for step, flag in zip(steps, flags) if flag)
        odd = sum(step[1] for step, flag in zip(steps, flags) if flag)
        chip = (me ^ (even + core * (odd - even))) >> 1
        other = list(flags)
        other[first], other[second] = flags[second], flags[first]
        place = sum(flag << k for k, flag in enumerate(other[:-1]))
        mine = (received if flags[-1] else held)[j % (1 << (depth - 1)), start : start + taps]
        theirs = (far if other[-1] else near)[place, start : start + taps]
        mine, theirs = mine.astype(F32), theirs.astype(F32)
        low, high = jnp.where(core == 0, mine, theirs), jnp.where(core == 0, theirs, mine)
        both = jnp.concatenate([low, high], axis=1).astype(BF16)
        row = pl.multiple_of(chip * (2 * block), 2 * block)
        for tap in range(taps):
            kernel[pl.ds(row, 2 * block), tap * inner : (tap + 1) * inner] = both[tap]


def conv_body(counts, layouts, *refs):
    levels = len(layouts)
    refs = list(refs)
    xs, refs = refs[:levels], refs[levels:]
    parts, refs = refs[:counts], refs[counts:]
    outs, stats, kernels = refs[:levels], refs[levels], refs[levels + 1 :]
    me = lax.axis_index("dp") * lax.axis_size("space") + lax.axis_index("space")
    for level in range(levels):
        x, out, kernel = xs[level], outs[level], kernels[level]
        first, last, start, steps, places = layouts[level]
        inner = x.shape[3] // 3
        lay_out(kernel, parts[first:last], start, steps, places, me, kernel.shape[1] // inner)
        images, rows, width, outer = out.shape
        area = rows * width
        group = max(1, min(images, 512 // area))
        while images % group:
            group -= 1
        for b in range(0, images, group):
            wide = jnp.concatenate(
                [x[b : b + group, a : a + rows].reshape(group * area, 3 * inner) for a in range(3)],
                axis=1,
            )
            value = lax.dot_general(
                wide, kernel[...], (((1,), (1,)), ((), ())), preferred_element_type=F32
            )
            out[b : b + group] = value.reshape(group, rows, width, outer)
            for i in range(group):
                mine = value[i * area : (i + 1) * area]
                mean = jnp.sum(mine, axis=0, keepdims=True) * (1.0 / area)
                deviation = mine - mean
                line = level * 2 * images + b + i
                stats[line : line + 1] = mean
                stats[line + images : line + images + 1] = jnp.sum(
                    deviation * deviation, axis=0, keepdims=True
                )


def convolve(xs, weights, outer):
    inner = xs[0].shape[3] // 3
    outs = [
        jax.ShapeDtypeStruct((x.shape[0], x.shape[1] - 2, x.shape[2], outer), F32) for x in xs
    ]
    flops = sum(2 * o.size * 9 * inner for o in outs)
    outs.append(jax.ShapeDtypeStruct((2 * xs[0].shape[0] * len(xs), outer), F32))
    arrays, layouts, before = [], [], None
    for parts, start, steps, places in weights:
        if parts is not before:
            arrays.extend(parts)
        before = parts
        layouts.append((len(arrays) - len(parts), len(arrays), start, steps, places))
    body = functools.partial(conv_body, len(arrays), layouts)
    ins = list(xs) + arrays
    scratch = [pltpu.VMEM((outer, 9 * inner), BF16) for _ in xs]
    result = call(body, outs, ins, scratch, flops)
    return result[:-1], result[-1]


def group_sums(values, size):
    lanes = values.shape[1]
    lane = lax.broadcasted_iota(jnp.int32, values.shape, 1)
    step = 1
    while step < size:
        up, down = pltpu.roll(values, lanes - step, 1), pltpu.roll(values, step, 1)
        values = values + jnp.where((lane & step) == 0, up, down)
        step *= 2
    return values


def norm_body(levels, pieces, *refs):
    refs = list(refs)
    xs, refs = refs[:levels], refs[levels:]
    affine, refs = refs[: 2 * levels], refs[2 * levels :]
    stats, refs = refs[:pieces], refs[pieces:]
    outs, refs = refs[:levels], refs[levels:]
    ys, sems = refs[:levels], refs[levels]
    images = xs[0].shape[0]
    channels = xs[0].shape[3]
    size = channels // G
    strips = [s[i] for s in stats for i in range(s.shape[0])]
    count = len(strips) * size
    total = group_sums(functools.reduce(jnp.add, strips), size)
    centers = total * (1.0 / count)
    apart = [(s - centers) for s in strips]
    between = group_sums(functools.reduce(jnp.add, [a * a for a in apart]), size)
    copies = []
    for level in range(levels):
        x, y = xs[level], ys[level]
        area = x.shape[1] * x.shape[2]
        first = level * 2 * images
        center = centers[first : first + images]
        spread = (
            total[first + images : first + 2 * images] + between[first : first + images] * area
        ) * (1.0 / (count * area))
        scale = lax.rsqrt(spread + EPSILON) * affine[2 * level][...]
        shift = affine[2 * level + 1][...]
        for b in range(images):
            flat = x[b].reshape(area, channels)
            line = (flat - center[b : b + 1]) * scale[b : b + 1] + shift
            y[b] = line.reshape(x.shape[1:])
            copy = pltpu.make_async_copy(y.at[b], outs[level].at[b], sems.at[level * images + b])
            copy.start()
            copies.append(copy)
    for copy in copies:
        copy.wait()


def normalize(xs, affine, stats):
    outs = [jax.ShapeDtypeStruct(x.shape, F32) for x in xs]
    ins = list(xs) + list(affine) + list(stats)
    scratch = [pltpu.VMEM(x.shape, F32) for x in xs]
    scratch.append(pltpu.SemaphoreType.DMA((len(xs) * xs[0].shape[0],)))
    body = functools.partial(norm_body, len(xs), len(stats))
    return call(
        body, outs, ins, scratch, 8 * sum(x.size for x in xs), out_specs=[ANY] * len(outs)
    )


def local(l3, l4, l5, w3, w4, w5, gain3, shift3, gain4, shift4, gain5, shift5):
    weights = weight_parts([w3, w4, w5])
    outer = shift3.shape[0]
    before, after = halos(l3, l4, l5)
    x3, x4, x5 = prepare(l3, l4, l5, before, after)
    (f3,), stats3 = convolve([x3], weights[:1], outer)
    (f4, f5), stats45 = convolve([x4, x5], weights[1:], outer)
    stats = statistics_of_all(joined(stats3, stats45))
    affine = [a[None] for a in (gain3, shift3, gain4, shift4, gain5, shift5)]
    return tuple(normalize([f3, f4, f5], affine, stats))


def solution(mesh):
    image = P("dp", "space", None, None)
    weight = P(None, None, None, AXES)
    return jax.shard_map(
        local,
        mesh=mesh,
        in_specs=(image,) * 3 + (weight,) * 3 + (P(),) * 6,
        out_specs=(image,) * 3,
        check_vma=False,
    )
```

```python
import functools

import jax
import jax.numpy as jnp
from jax import lax
from jax.experimental import pallas as pl
from jax.experimental.pallas import tpu as pltpu
from jax.sharding import PartitionSpec as P


G = 32
EPSILON = 1e-05
LANES = 128
AXES = ("dp", "space")
F32 = jnp.float32
BF16 = jnp.bfloat16
VMEM = pl.BlockSpec(memory_space=pltpu.VMEM)
ANY = pl.BlockSpec(memory_space=pl.ANY)


def exchange(array, axes, size, masks):
    return lax.ppermute(array, axes, [(i, i ^ masks[i % 2]) for i in range(size)])


def join_body(*refs):
    target, start = refs[-1], 0
    for ref in refs[:-1]:
        target[start : start + ref.shape[0]] = ref[...]
        start += ref.shape[0]


def joined(*arrays):
    count = sum(a.shape[0] for a in arrays)
    out = jax.ShapeDtypeStruct((count,) + arrays[0].shape[1:], arrays[0].dtype)
    return call(join_body, [out], list(arrays), [], out.size, room=1)[0]


def halve_body(cut, first, second, *targets):
    for target, lo, hi in ((targets[0], 0, cut), (targets[1], cut, first.shape[1])):
        count = first.shape[0]
        target[:count] = first[:, lo:hi]
        target[count:] = second[:, lo:hi]


def halved(first, second, cut):
    count, length = first.shape[:2]
    outs = [
        jax.ShapeDtypeStruct((2 * count, n) + first.shape[2:], first.dtype)
        for n in (cut, length - cut)
    ]
    return call(functools.partial(halve_body, cut), outs, [first, second], [], 2 * first.size, room=1)


def gathered_in_chains(together, lengths, bits):
    size = lax.axis_size(AXES)
    lead, (p, q, r) = bits[:-3], bits[-3:]
    for k, bit in enumerate(lead):
        received = exchange(together, AXES, size, (bit, bit))
        if k + 1 < len(lead):
            together = joined(together, received)
    chunks = halved(together, received, lengths[0])
    orders = [[(q, r), (p, p), (r, q)], [(p, p), (q, r), (r, q)]]
    swapped = [(len(lead) + 0, len(lead) + 2), (len(lead) + 1, len(lead) + 2)]
    result = []
    result = []
    for chunk, order, places, members in zip(chunks, orders, swapped, (lengths[:1], lengths[1:])):
        received = exchange(chunk, AXES, size, order[0])
        chunk = joined(chunk, received)
        received = exchange(chunk, AXES, size, order[1])
        if len(members) == 1:
            pieces = [joined(chunk, received)]
        else:
            pieces = halved(chunk, received, members[0])
        steps = [(bit, bit) for bit in lead] + order
        for piece in pieces:
            last = exchange(piece, AXES, size, order[2])
            near = exchange(piece, AXES, size, (1, 1))
            far = exchange(last, AXES, size, (1, 1))
            result.append(([piece, last, near, far], 0, steps, places))
    return result


def weight_parts(weights):
    size = lax.axis_size(AXES)
    shards = []
    for weight in weights:
        rows, columns, inner, outer = weight.shape
        shards.append(jnp.transpose(weight, (0, 1, 3, 2)).reshape(rows * columns, outer, inner))
    bits = [1 << k for k in range(size.bit_length() - 1)][::-1][:-1]
    paired = lax.axis_size("space") % 2 == 0
    if paired and size == 2 << len(bits) and len(bits) > 3 and shards[0].shape[1] == 8:
        together = jnp.concatenate(shards, axis=0)[None]
        return gathered_in_chains(together, [s.shape[0] for s in shards], bits)
    return [
        ([lax.all_gather(shard, AXES, axis=1, tiled=True)], 0, None, None) for shard in shards
    ]


def starts_of(*levels):
    starts, start = [], 0
    for level in levels:
        starts.append(start)
        start += level.shape[2]
    return starts


def edges_body(l3, l4, l5, top, bottom, sems):
    copies = []
    for source, start in zip((l3, l4, l5), starts_of(l3, l4, l5)):
        rows, width = source.shape[1:3]
        for target, row in ((top, 0), (bottom, rows - 1)):
            copies.append(
                pltpu.make_async_copy(
                    source.at[:, row], target.at[:, start : start + width], sems.at[len(copies)]
                )
            )
            copies[-1].start()
    for copy in copies:
        copy.wait()


def halos(*levels):
    count = lax.axis_size("space")
    ahead = [(i, i + 1) for i in range(count - 1)]
    width = sum(a.shape[2] for a in levels)
    edge = jax.ShapeDtypeStruct((levels[0].shape[0], width, levels[0].shape[3]), BF16)
    kept = [pltpu.with_memory_space_constraint(a, pltpu.HBM) for a in levels]
    scratch = [pltpu.SemaphoreType.DMA((2 * len(levels),))]
    top, bottom = call(
        edges_body, [edge, edge], kept, scratch, edge.size, in_specs=[ANY] * len(kept), room=1
    )
    before = lax.ppermute(bottom, "space", ahead)
    after = lax.ppermute(top, "space", [(j, i) for i, j in ahead])
    return before, after


def statistics_of_all(own):
    size = lax.axis_size("space")
    bits = [1 << k for k in range(size.bit_length() - 1)]
    if size != 1 << len(bits):
        return [lax.all_gather(own, "space")]
    held = [own[None]]
    for start in range(0, len(bits), 2) if len(bits) % 2 == 0 else [-1] + list(range(1, len(bits), 2)):
        some = bits[max(start, 0) : start + 2]
        whole = held[0] if len(held) == 1 else joined(*held)
        masks = some if len(some) == 1 else [some[0] | some[1]] + some
        held = [whole] + [exchange(whole, "space", size, (m, m)) for m in masks]
    return held


def call(body, outs, ins, scratch, flops, in_specs=None, out_specs=None, room=8):
    moved = sum(a.size * a.dtype.itemsize for a in list(outs) + list(ins))
    return pl.pallas_call(
        body,
        out_shape=outs,
        in_specs=in_specs or [VMEM] * len(ins),
        out_specs=out_specs or [VMEM] * len(outs),
        scratch_shapes=scratch,
        compiler_params=pltpu.CompilerParams(vmem_limit_bytes=room << 20),
        cost_estimate=pl.CostEstimate(flops=flops, bytes_accessed=moved, transcendentals=0),
    )(*ins)


def stretched(scratch, values):
    rows = values.shape[0]
    pieces = []
    for k in range(scratch.shape[0]):
        piece = values[:, k * LANES : (k + 1) * LANES]
        scratch[k, pl.ds(0, rows, stride=2), :] = piece
        scratch[k, pl.ds(1, rows, stride=2), :] = piece
        pieces.append(scratch[k])
    return jnp.concatenate(pieces, axis=1)


def prepare_body(l3, l4, l5, before, after, x3, x4, x5, fine, middle):
    images, rows5 = l5.shape[0], l5.shape[1]
    channels = l5.shape[3]

    def put(target, b, row, wide):
        width = wide.shape[0]
        column = lax.broadcasted_iota(jnp.int32, wide.shape, 0)
        left = jnp.where(column == 0, 0.0, pltpu.roll(wide, 1, 0))
        right = jnp.where(column == width - 1, 0.0, pltpu.roll(wide, width - 1, 0))
        for k, piece in enumerate((left, wide, right)):
            target[b, row, :, k * channels : (k + 1) * channels] = piece.astype(BF16)

    def rounded(values):
        return values.astype(BF16).astype(F32)

    starts = starts_of(l3, l4, l5)
    for b in range(images):
        for side, halo in enumerate((before, after)):
            rows = []
            for source, start in zip((l3, l4, l5), starts):
                rows.append(halo[b, start : start + source.shape[2]].astype(F32))
            put(x5, b, side * (x5.shape[1] - 1), rows[2])
            v4 = rounded(rows[1] + stretched(middle, rows[2]))
            put(x4, b, side * (x4.shape[1] - 1), v4)
            put(x3, b, side * (x3.shape[1] - 1), rounded(rows[0] + stretched(fine, v4)))
        for r5 in range(rows5):
            v5 = l5[b, r5].astype(F32)
            put(x5, b, 1 + r5, v5)
            up5 = stretched(middle, v5)
            for r4 in (2 * r5, 2 * r5 + 1):
                v4 = rounded(l4[b, r4].astype(F32) + up5)
                put(x4, b, 1 + r4, v4)
                up4 = stretched(fine, v4)
                for r3 in (2 * r4, 2 * r4 + 1):
                    put(x3, b, 1 + r3, rounded(l3[b, r3].astype(F32) + up4))


def prepare(l3, l4, l5, before, after):
    levels = (l3, l4, l5)
    channels = l3.shape[3]
    outs = [
        jax.ShapeDtypeStruct((a.shape[0], a.shape[1] + 2, a.shape[2], 3 * channels), BF16)
        for a in levels
    ]
    scratch = [pltpu.VMEM((channels // LANES, a.shape[2], LANES), F32) for a in (l3, l4)]
    ins = [l3, l4, l5, before, after]
    return call(prepare_body, outs, ins, scratch, 8 * sum(o.size for o in outs), room=2)


def lay_out(kernel, parts, start, steps, places, me, taps):
    inner = kernel.shape[1] // taps
    if steps is None:
        for tap in range(taps):
            kernel[:, tap * inner : (tap + 1) * inner] = parts[0][tap]
        return
    held, received, near, far = parts
    block = held.shape[2]
    core = me & 1
    depth = len(steps)
    first, second = places
    for j in range(1 << depth):
        flags = [(j >> k) & 1 for k in range(depth)]
        even = sum(step[0] for step, flag in zip(steps, flags) if flag)
        odd = sum(step[1] for step, flag in zip(steps, flags) if flag)
        chip = (me ^ (even + core * (odd - even))) >> 1
        other = list(flags)
        other[first], other[second] = flags[second], flags[first]
        place = sum(flag << k for k, flag in enumerate(other[:-1]))
        mine = (received if flags[-1] else held)[j % (1 << (depth - 1)), start : start + taps]
        theirs = (far if other[-1] else near)[place, start : start + taps]
        mine, theirs = mine.astype(F32), theirs.astype(F32)
        low, high = jnp.where(core == 0, mine, theirs), jnp.where(core == 0, theirs, mine)
        both = jnp.concatenate([low, high], axis=1).astype(BF16)
        row = pl.multiple_of(chip * (2 * block), 2 * block)
        for tap in range(taps):
            kernel[pl.ds(row, 2 * block), tap * inner : (tap + 1) * inner] = both[tap]


def conv_body(counts, layouts, *refs):
    levels = len(layouts)
    refs = list(refs)
    xs, refs = refs[:levels], refs[levels:]
    parts, refs = refs[:counts], refs[counts:]
    outs, stats, kernels = refs[:levels], refs[levels], refs[levels + 1 :]
    me = lax.axis_index("dp") * lax.axis_size("space") + lax.axis_index("space")
    for level in range(levels):
        x, out, kernel = xs[level], outs[level], kernels[level]
        first, last, start, steps, places = layouts[level]
        inner = x.shape[3] // 3
        lay_out(kernel, parts[first:last], start, steps, places, me, kernel.shape[1] // inner)
        images, rows, width, outer = out.shape
        area = rows * width
        group = max(1, min(images, 512 // area))
        while images % group:
            group -= 1
        for b in range(0, images, group):
            wide = jnp.concatenate(
                [x[b : b + group, a : a + rows].reshape(group * area, 3 * inner) for a in range(3)],
                axis=1,
            )
            value = lax.dot_general(
                wide, kernel[...], (((1,), (1,)), ((), ())), preferred_element_type=F32
            )
            out[b : b + group] = value.reshape(group, rows, width, outer)
            for i in range(group):
                mine = value[i * area : (i + 1) * area]
                mean = jnp.sum(mine, axis=0, keepdims=True) * (1.0 / area)
                deviation = mine - mean
                line = level * 2 * images + b + i
                stats[line : line + 1] = mean
                stats[line + images : line + images + 1] = jnp.sum(
                    deviation * deviation, axis=0, keepdims=True
                )


def convolve(xs, weights, outer):
    inner = xs[0].shape[3] // 3
    outs = [
        jax.ShapeDtypeStruct((x.shape[0], x.shape[1] - 2, x.shape[2], outer), F32) for x in xs
    ]
    flops = sum(2 * o.size * 9 * inner for o in outs)
    outs.append(jax.ShapeDtypeStruct((2 * xs[0].shape[0] * len(xs), outer), F32))
    arrays, layouts, before = [], [], None
    for parts, start, steps, places in weights:
        if parts is not before:
            arrays.extend(parts)
        before = parts
        layouts.append((len(arrays) - len(parts), len(arrays), start, steps, places))
    body = functools.partial(conv_body, len(arrays), layouts)
    ins = list(xs) + arrays
    scratch = [pltpu.VMEM((outer, 9 * inner), BF16) for _ in xs]
    result = call(body, outs, ins, scratch, flops)
    return result[:-1], result[-1]


def group_sums(values, size):
    lanes = values.shape[1]
    lane = lax.broadcasted_iota(jnp.int32, values.shape, 1)
    step = 1
    while step < size:
        up, down = pltpu.roll(values, lanes - step, 1), pltpu.roll(values, step, 1)
        values = values + jnp.where((lane & step) == 0, up, down)
        step *= 2
    return values


def norm_body(levels, pieces, *refs):
    refs = list(refs)
    xs, refs = refs[:levels], refs[levels:]
    affine, refs = refs[: 2 * levels], refs[2 * levels :]
    stats, refs = refs[:pieces], refs[pieces:]
    outs, refs = refs[:levels], refs[levels:]
    ys, sems = refs[:levels], refs[levels]
    images = xs[0].shape[0]
    channels = xs[0].shape[3]
    size = channels // G
    strips = [s[i] for s in stats for i in range(s.shape[0])]
    count = len(strips) * size
    total = group_sums(functools.reduce(jnp.add, strips), size)
    centers = total * (1.0 / count)
    apart = [(s - centers) for s in strips]
    between = group_sums(functools.reduce(jnp.add, [a * a for a in apart]), size)
    copies = []
    for level in range(levels):
        x, y = xs[level], ys[level]
        area = x.shape[1] * x.shape[2]
        first = level * 2 * images
        center = centers[first : first + images]
        spread = (
            total[first + images : first + 2 * images] + between[first : first + images] * area
        ) * (1.0 / (count * area))
        scale = lax.rsqrt(spread + EPSILON) * affine[2 * level][...]
        shift = affine[2 * level + 1][...]
        for b in range(images):
            flat = x[b].reshape(area, channels)
            line = (flat - center[b : b + 1]) * scale[b : b + 1] + shift
            y[b] = line.reshape(x.shape[1:])
            copy = pltpu.make_async_copy(y.at[b], outs[level].at[b], sems.at[level * images + b])
            copy.start()
            copies.append(copy)
    for copy in copies:
        copy.wait()


def normalize(xs, affine, stats):
    outs = [jax.ShapeDtypeStruct(x.shape, F32) for x in xs]
    ins = list(xs) + list(affine) + list(stats)
    scratch = [pltpu.VMEM(x.shape, F32) for x in xs]
    scratch.append(pltpu.SemaphoreType.DMA((len(xs) * xs[0].shape[0],)))
    body = functools.partial(norm_body, len(xs), len(stats))
    return call(
        body, outs, ins, scratch, 8 * sum(x.size for x in xs), out_specs=[ANY] * len(outs)
    )


def local(l3, l4, l5, w3, w4, w5, gain3, shift3, gain4, shift4, gain5, shift5):
    weights = weight_parts([w3, w4, w5])
    outer = shift3.shape[0]
    before, after = halos(l3, l4, l5)
    x3, x4, x5 = prepare(l3, l4, l5, before, after)
    (f3,), stats3 = convolve([x3], weights[:1], outer)
    (f4,), stats4 = convolve([x4], weights[1:2], outer)
    (f5,), stats5 = convolve([x5], weights[2:], outer)
    stats = statistics_of_all(joined(stats3, stats4, stats5))
    affine = [a[None] for a in (gain3, shift3, gain4, shift4, gain5, shift5)]
    return tuple(normalize([f3, f4, f5], affine, stats))


def solution(mesh):
    image = P("dp", "space", None, None)
    weight = P(None, None, None, AXES)
    return jax.shard_map(
        local,
        mesh=mesh,
        in_specs=(image,) * 3 + (weight,) * 3 + (P(),) * 6,
        out_specs=(image,) * 3,
        check_vma=False,
    )
```
